16 devices in a mesh: dp: 1, tp: 16 (over x, y, z, core).
Axes of the slice: x: 2, y: 2, z: 2, core: 2. Of those that a mesh axis runs over, the one named last changes fastest.
Arguments:
- x: bfloat16 [4096, 4608], P(('dp', 'tp'))
- gain_a: bfloat16 [4608], replicated
- wq: bfloat16 [4608, 4096], P(None, 'tp')
- wk: bfloat16 [4608, 2048], P(None, 'tp')
- wv: bfloat16 [4608, 2048], P(None, 'tp')
- wo: bfloat16 [4096, 4608], P('tp')
- gain_m: bfloat16 [4608], replicated
- w_gate: bfloat16 [4608, 36864], P(None, 'tp')
- w_up: bfloat16 [4608, 36864], P(None, 'tp')
- w_down: bfloat16 [36864, 4608], P('tp')
Outputs:
- output: bfloat16 [4096, 4608], P(('dp', 'tp'))
All inputs are finite; a program needn't handle non-finite values.
Results may differ from the reference program's by a relative error of at most 0.017.
Values are sent between devices in bfloat16 or wider.
A program may use at most 2 GiB of HBM per device.

```python
import jax
import jax.numpy as jnp
from jax import lax

ROWS = 4096
D = 4608
HEADS = 32
KV_HEADS = 16
HEAD = 128
FF = 36864
THETA = 10000


def setup_inputs(seed: int = 0, part: int = 0) -> dict:
    kx, kn, kq, kk, kv, ko, km, kg, ku, kd = jax.random.split(jax.random.key(seed), 10)

    def weights(key, rows, columns):
        return jax.random.normal(key, (rows, columns), jnp.float32) * rows**-0.5

    drawn = {
        "x": jax.random.normal(jax.random.fold_in(kx, part), (ROWS, D), jnp.float32),
        "gain_a": 1 + 0.1 * jax.random.normal(kn, (D,), jnp.float32),
        "wq": 2 * weights(kq, D, HEADS * HEAD),
        "wk": 2 * weights(kk, D, KV_HEADS * HEAD),
        "wv": 4 * weights(kv, D, KV_HEADS * HEAD),
        "wo": weights(ko, HEADS * HEAD, D),
        "gain_m": 1 + 0.1 * jax.random.normal(km, (D,), jnp.float32),
        "w_gate": weights(kg, D, FF),
        "w_up": weights(ku, D, FF),
        "w_down": 2 * weights(kd, FF, D),
    }
    return {k: v.astype(jnp.bfloat16) for k, v in drawn.items()}


def normed(x, gain):
    wide = x.astype(jnp.float32)
    scale = lax.rsqrt(jnp.mean(wide * wide, -1, keepdims=True) + 1e-6)
    return (wide * scale * gain.astype(jnp.float32)).astype(jnp.bfloat16)


def turned(t, place, theta):
    half = t.shape[-1] // 2
    angle = place.astype(jnp.float32)[:, None] * theta ** (-jnp.arange(half, dtype=jnp.float32) / half)
    cos, sin = jnp.cos(angle)[:, None], jnp.sin(angle)[:, None]
    a, b = t[..., :half].astype(jnp.float32), t[..., half:].astype(jnp.float32)
    return jnp.concatenate([a * cos - b * sin, b * cos + a * sin], -1).astype(jnp.bfloat16)


def matmul(a, w):
    return jnp.dot(a, w, preferred_element_type=jnp.float32).astype(jnp.bfloat16)


def einsum(form, a, b):
    return jnp.einsum(form, a.astype(jnp.float32), b.astype(jnp.float32))


def attention(q, k, v):
    scores = einsum("tgsd,ugd->gstu", q, k) * q.shape[-1] ** -0.5
    token = jnp.arange(q.shape[0])
    scores = jnp.where(token[:, None] >= token, scores, -jnp.inf)
    weights = jax.nn.softmax(scores, -1).astype(jnp.bfloat16)
    return einsum("gstu,ugd->tgsd", weights, v).astype(jnp.bfloat16)


def reference(x, gain_a, wq, wk, wv, wo, gain_m, w_gate, w_up, w_down):
    a, place = normed(x, gain_a), jnp.arange(ROWS)
    q = turned(matmul(a, wq).reshape(ROWS, HEADS, HEAD), place, THETA).reshape(ROWS, KV_HEADS, -1, HEAD)
    k = turned(matmul(a, wk).reshape(ROWS, KV_HEADS, HEAD), place, THETA)
    v = matmul(a, wv).reshape(ROWS, KV_HEADS, HEAD)
    seen = attention(q, k, v).reshape(ROWS, HEADS * HEAD)
    h = (x.astype(jnp.float32) + jnp.dot(seen, wo, preferred_element_type=jnp.float32)).astype(jnp.bfloat16)
    b = normed(h, gain_m)
    gate = jnp.dot(b, w_gate, preferred_element_type=jnp.float32)
    up = jnp.dot(b, w_up, preferred_element_type=jnp.float32)
    hidden = (jax.nn.silu(gate) * up).astype(jnp.bfloat16)
    return (h.astype(jnp.float32) + jnp.dot(hidden, w_down, preferred_element_type=jnp.float32)).astype(jnp.bfloat16)
```

```python
import functools

import jax
import jax.numpy as jnp
from jax import lax
from jax.experimental import pallas as pl
from jax.experimental.pallas import tpu as pltpu
from jax.sharding import PartitionSpec as P

NEG = -1e30
HIDDEN = 2 * NEG
LOG2E = 1.4426950408889634
VMEM = 67043328
HEAD = 128
THETA = 10000
MESH_AXIS = "tp"
PARTS = 3
ROUNDS = 8
STEPS = PARTS * ROUNDS


def normed(x, gain):
    wide = x.astype(jnp.float32)
    scale = lax.rsqrt(jnp.mean(wide * wide, -1, keepdims=True) + 1e-6)
    return (wide * scale * gain.astype(jnp.float32)).astype(jnp.bfloat16)


def _bit(part, k):
    axis = lax.rem(part + k, 3)
    return 4 - 2 * axis + (axis * (axis - 1)) // 2


def _flip(v, bit, on=1):
    return v + on * bit * (1 - 2 * lax.rem(v // bit, 2))


def _dot(a, b, ca, cb):
    return lax.dot_general(a, b, (((ca,), (cb,)), ((), ())), preferred_element_type=jnp.float32)


def _attention(seen_ref, block, q_v, k_v, vt_v, top_s, mix_s):
    heads, size = q_v.shape[0], q_v.shape[2]
    e = HEAD**-0.5 * LOG2E
    top_s[...] = jnp.full(top_s.shape, NEG, jnp.float32)
    mix_s[...] = jnp.zeros(mix_s.shape, jnp.float32)

    def keys(j, masked):
        scores = [_dot(k_v[j], q_v[i, block], 1, 1) for i in range(heads)]
        weights, keeps = [], []
        for i, s in enumerate(scores):
            if masked:
                s = jnp.where(lax.broadcasted_iota(jnp.int32, s.shape, 1) >= lax.broadcasted_iota(jnp.int32, s.shape, 0), s, HIDDEN)
            old = top_s[i]
            top = jnp.maximum(old, s.max(axis=0, keepdims=True))
            top_s[i] = top
            weights.append(jnp.exp2((s - top) * e).astype(jnp.bfloat16))
            keeps.append(jnp.exp2((old - top) * e))
        for i, (p, keep) in enumerate(zip(weights, keeps)):
            mix_s[i] = mix_s[i] * keep + _dot(vt_v[j], p, 1, 0)

    lax.fori_loop(0, block, lambda j, _: keys(j, False), None)
    keys(block, True)
    for i in range(heads):
        seen_ref[:, i * HEAD : (i + 1) * HEAD] = (mix_s[i, :HEAD, :] * (1 / mix_s[i, HEAD : HEAD + 1, :])).T.astype(jnp.bfloat16)


def _summed(cols, attending, *refs):
    if attending:
        q_ref, k_ref, v_ref, *refs = refs
        w_ref, out_ref, q_v, k_v, v_v, vt_v, top_s, mix_s, seen_v, qkv_sem, *refs = refs
    else:
        a_ref, w_ref, out_ref, a_v, a_sem, *refs = refs
    w_v, acc, stage, near, send, recv, w_sem, stage_sem, near_sem, send_sem, recv_sem, out_sem, free_sem = refs
    me = lax.axis_index(MESH_AXIS)
    core, chip = lax.rem(me, 2), me // 2
    other = me + 1 - 2 * core
    half = acc.shape[1]
    width = acc.shape[2]

    def to(device):
        return dict(device_id={MESH_AXIS: device}, device_id_type=pl.DeviceIdType.MESH)

    barrier = pltpu.get_barrier_semaphore()
    pl.semaphore_signal(barrier, inc=1, **to(other))
    for bit in (4, 2, 1):
        pl.semaphore_signal(barrier, inc=1, **to(_flip(chip, bit) * 2 + core))

    def w_copy(part):
        columns = pl.ds(pl.multiple_of(part * width, width), width)
        return pltpu.make_async_copy(w_ref.at[:, columns], w_v.at[:, columns], w_sem.at[part])

    def dest(t):
        part, left = lax.rem(t, PARTS), 7 - t // PARTS
        at = _flip(chip, _bit(part, 0), left // 4)
        at = _flip(at, _bit(part, 1), lax.rem(left // 2, 2))
        return _flip(at, _bit(part, 2), lax.rem(left, 2))

    def a_copy(t):
        slot = lax.rem(t, 2)
        return pltpu.make_async_copy(a_ref.at[pl.ds(dest(t) * 2, 2)], a_v.at[slot], a_sem.at[slot])

    def stage_copy(t):
        slot, place = lax.rem(t, 2), lax.rem(t, 6)
        return pltpu.make_async_remote_copy(src_ref=stage.at[slot], dst_ref=near.at[place], send_sem=stage_sem.at[slot],
                                            recv_sem=near_sem.at[place], **to(other))

    def send_copy(t):
        part, rnd, slot = lax.rem(t, PARTS), t // PARTS, lax.rem(t, 12)
        target = _flip(chip, _bit(part, rnd // 4 + rnd // 6)) * 2 + core
        return pltpu.make_async_remote_copy(src_ref=send.at[slot], dst_ref=recv.at[t], send_sem=send_sem.at[slot],
                                            recv_sem=recv_sem.at[t], **to(target))

    def out_copy(part):
        return pltpu.make_async_copy(send.at[lax.rem(part + 21, 12)], out_ref.at[:, pl.ds(pl.multiple_of(part * width, width), width)], out_sem.at[part])

    if attending:
        loads = [pltpu.make_async_copy(src, dst, qkv_sem.at[i]) for i, (src, dst) in enumerate(((q_ref, q_v), (k_ref, k_v), (v_ref, v_v)))]
        for copy in loads:
            copy.start()
    for part in range(PARTS):
        w_copy(part).start()
        if part < 2 and not attending:
            a_copy(part).start()
    if attending:
        for copy in loads:
            copy.wait()
        ones = jnp.ones((8, vt_v.shape[2]), jnp.bfloat16)

        def turn(j, _):
            vt_v[j] = jnp.concatenate([v_v[j].T, ones], axis=0)

        lax.fori_loop(0, ROUNDS, turn, None)
    pl.semaphore_wait(barrier, 4)

    def product(t):
        part, slot = lax.rem(t, PARTS), lax.rem(t, 2)

        @pl.when(t < PARTS)
        def _():
            w_copy(part).wait()

        if not attending:
            a_copy(t).wait()

        @pl.when(t >= 2)
        def _():
            stage_copy(t - 2).wait_send()

        def tile(i, _):
            a = seen_v[dest(t)] if attending else a_v[slot].reshape(2 * half, a_v.shape[3])
            here = pl.ds(pl.multiple_of(i * cols, cols), cols)
            got = jnp.dot(a, w_v[:, pl.ds(pl.multiple_of(part * width + i * cols, cols), cols)], preferred_element_type=jnp.float32)
            low, high = got[:half], got[half:]
            acc[slot, :, here] = jnp.where(core == 0, low, high)
            stage[slot, :, here] = jnp.where(core == 0, high, low).astype(jnp.bfloat16)

        lax.fori_loop(0, width // cols, tile, None)

        if not attending:
            @pl.when(t + 2 < STEPS)
            def _():
                a_copy(t + 2).start()

        @pl.when(t >= 6)
        def _():
            pl.semaphore_wait(free_sem, 1)

        stage_copy(t).start()

    def gathered(t):
        part, rnd, slot, place = lax.rem(t, PARTS), t // PARTS, lax.rem(t, 12), lax.rem(t, 6)
        stage_copy(t).wait_recv()

        @pl.when(t >= 12)
        def _():
            send_copy(t - 12).wait_send()

        def add(froms):
            for s in froms:
                send_copy(s).wait_recv()

            def some(i, _):
                rows = pl.ds(pl.multiple_of(i * 16, 16), 16)
                total = acc[lax.rem(t, 2), rows, :] + near[place, rows, :].astype(jnp.float32)
                for s in froms:
                    total += recv[s, rows, :].astype(jnp.float32)
                send[slot, rows, :] = total.astype(jnp.bfloat16)

            lax.fori_loop(0, half // 16, some, None)

        @pl.when(rnd < 4)
        def _():
            add([])

        @pl.when((rnd >= 4) & (rnd < 6))
        def _():
            add([t - 12])

        @pl.when(rnd == 6)
        def _():
            add([t - 12, t - 6])

        @pl.when(rnd == 7)
        def _():
            add([t - 12, t - 6, t - 3])

        @pl.when(t < STEPS - 6)
        def _():
            pl.semaphore_signal(free_sem, inc=1, **to(other))

        @pl.when(rnd < 7)
        def _():
            send_copy(t).start()

        @pl.when(rnd == 7)
        def _():
            out_copy(part).start()

    def first(t):
        return (t == 0) | ((t >= 3) & (t < 6)) | ((t >= 9) & (t < 12)) | (t == 21)

    def step(t, _):
        @pl.when((t >= 0) & (t < STEPS))
        def _():
            product(t)

        late = t >= 1
        if attending:
            late = late & jnp.logical_not(first(t))

        @pl.when(late)
        def _():
            gathered(t - 1)

        if attending:
            @pl.when(first(t + 1))
            def _():
                @pl.when(t >= 0)
                def _():
                    gathered(t)

                _attention(seen_v.at[dest(t + 1)], dest(t + 1), q_v, k_v, vt_v, top_s, mix_s)

    lax.fori_loop(-1 if attending else 0, STEPS + 1, step, None)
    for t in (STEPS - 2, STEPS - 1):
        stage_copy(t).wait_send()
    for t in range(12, 21):
        send_copy(t).wait_send()
    for part in range(PARTS):
        out_copy(part).wait()


def summed(given, w, collective_id, cols):
    rows, depth, columns = given[0].shape[-2], w.shape[0], w.shape[1]
    piece = (rows, columns // PARTS)
    anywhere = pl.BlockSpec(memory_space=pl.ANY)
    dma = pltpu.SemaphoreType.DMA
    attending = len(given) == 3
    if attending:
        heads, block = given[0].shape[0], 2 * rows
        shapes = ((heads, ROUNDS, block, HEAD), (ROUNDS, block, HEAD), (ROUNDS, block, HEAD))
        given = [t.reshape(shape) for t, shape in zip(given, shapes)]
        own = [pltpu.VMEM(shape, jnp.bfloat16) for shape in shapes]
        own += [pltpu.VMEM((ROUNDS, HEAD + 8, block), jnp.bfloat16), pltpu.VMEM((heads, 1, block), jnp.float32),
                pltpu.VMEM((heads, HEAD + 8, block), jnp.float32), pltpu.VMEM((ROUNDS, block, depth), jnp.bfloat16), dma((3,))]
    else:
        own = [pltpu.VMEM((2, 2, rows, depth), jnp.bfloat16), dma((2,))]
    return pl.pallas_call(
        functools.partial(_summed, cols, attending),
        out_shape=jax.ShapeDtypeStruct((rows, columns), jnp.bfloat16),
        in_specs=[anywhere] * (len(given) + 1),
        out_specs=anywhere,
        scratch_shapes=[
            *own,
            pltpu.VMEM((depth, columns), jnp.bfloat16),
            pltpu.VMEM((2, *piece), jnp.float32),
            pltpu.VMEM((2, *piece), jnp.bfloat16),
            pltpu.VMEM((6, *piece), jnp.bfloat16),
            pltpu.VMEM((12, *piece), jnp.bfloat16),
            pltpu.VMEM((21, *piece), jnp.bfloat16),
            dma((PARTS,)), dma((2,)), dma((6,)), dma((12,)), dma((21,)), dma((PARTS,)),
            pltpu.SemaphoreType.REGULAR,
        ],
        compiler_params=pltpu.CompilerParams(collective_id=collective_id, has_side_effects=True, vmem_limit_bytes=VMEM),
        cost_estimate=pl.CostEstimate(flops=2 * 16 * rows * depth * columns, bytes_accessed=2 * (16 * rows * depth + depth * columns), transcendentals=0),
    )(*given, w)


SENDS = (((), 0), ((), 1), ((), 2), ((0,), 1), ((0,), 2), ((1,), 2), ((0, 1), 2))
UNITS = ((0, 0), (0, 1), (4, 0), (2, 0), (1, 0), (4, 1), (2, 1), (1, 1), (6, 0), (3, 0), (5, 0), (7, 0), (6, 1), (3, 1), (5, 1), (7, 1))


def _fetched(tiles, work, load_weights, n_in, n_out, *refs):
    t_ref, ins = refs[0], refs[1:n_in]
    outs, all_ref = refs[n_in : n_in + n_out], refs[n_in + n_out]
    x_v, x_sem, send_sem, recv_sem, pair_send, pair_recv, out_sem, *scratch = refs[n_in + n_out + 1 :]
    me = lax.axis_index(MESH_AXIS)
    core, chip = lax.rem(me, 2), me // 2
    other = me + 1 - 2 * core
    rows, width = x_v.shape[2], t_ref.shape[1] // PARTS

    def to(device):
        return dict(device_id={MESH_AXIS: device}, device_id_type=pl.DeviceIdType.MESH)

    barrier = pltpu.get_barrier_semaphore()
    pl.semaphore_signal(barrier, inc=1, **to(other))
    for bit in (4, 2, 1):
        pl.semaphore_signal(barrier, inc=1, **to(_flip(chip, bit) * 2 + core))
    pl.semaphore_wait(barrier, 4)

    def link(part, half, i):
        way, axis = SENDS[i]
        bits = [(4, 2, 1)[(part + k) % 3] for k in range(3)]
        source = chip
        for k in way:
            source = _flip(source, bits[k])
        here, columns = pl.ds(half * rows, rows), pl.ds(part * width, width)
        place = all_ref.at[source * 2 + core, here, columns]
        return pltpu.make_async_remote_copy(src_ref=place if way else t_ref.at[here, columns], dst_ref=place, send_sem=send_sem.at[half, part, i],
                                            recv_sem=recv_sem.at[half, part, i], **to(_flip(chip, bits[axis]) * 2 + core))

    def pair(u):
        mask, half = UNITS[u]
        source = chip
        for bit in (4, 2, 1):
            source = _flip(source, bit, int(mask & bit != 0))
        here = pl.ds(half * rows, rows)
        place = all_ref.at[source * 2 + core, here]
        return pltpu.make_async_remote_copy(src_ref=place if mask else t_ref.at[here], dst_ref=place, send_sem=pair_send.at[u],
                                            recv_sem=pair_recv.at[u], **to(other))

    def start(half, *sends):
        for i in sends:
            for part in range(PARTS):
                link(part, half, i).start()

    def arrived(half, *sends):
        for i in sends:
            for part in range(PARTS):
                link(part, half, i).wait_recv()

    def pairs(*units):
        for u in units:
            pair(u).start()

    def before(u):
        if u == 2:
            arrived(0, 0, 1, 2)
            start(0, 3, 4, 5)
            pairs(2, 3, 4)
        if u == 5:
            arrived(1, 0, 1, 2)
            start(1, 3, 4, 5)
            pairs(5, 6, 7)
            arrived(0, 3)
            start(0, 6)
        if u == 7:
            arrived(1, 3)
            start(1, 6)
        if u == 8:
            arrived(0, 4, 5)
            pairs(8, 9, 10)
        if u == 11:
            arrived(0, 6)
            pairs(11)
        if u == 12:
            arrived(1, 4, 5)
            pairs(12, 13, 14)
        if u == 15:
            arrived(1, 6)
            pairs(15)

    def where(u):
        mask = half = 0
        for k, (m, h) in enumerate(UNITS):
            mask, half = jnp.where(u == k, m, mask), jnp.where(u == k, h, half)
        source = chip
        for bit in (4, 2, 1):
            source = _flip(source, bit, lax.rem(mask // bit, 2))
        return source, half

    def load(u, c, own=False):
        source, half = where(u)
        here = pl.ds(half * rows, rows)
        return pltpu.make_async_copy(t_ref.at[here] if own else all_ref.at[source * 2 + c, here], x_v.at[lax.rem(u, 2), c], x_sem.at[lax.rem(u, 2), c])

    def fetch(u):
        for k in range(len(UNITS)):
            @pl.when(u == k)
            def _():
                before(k)
                pair(k).wait_recv()

        for c in (0, 1):
            @pl.when((u < 2) & (core == c))
            def _():
                load(u, c, True).start()

            @pl.when((u >= 2) | (core != c))
            def _():
                load(u, c).start()

    start(0, 0, 1, 2)
    pairs(0, 1)
    start(1, 0, 1, 2)
    load_weights(ins, scratch)
    fetch(0)

    def step(s, _):
        u, i = s // tiles, lax.rem(s, tiles)

        @pl.when(i == 0)
        def _():
            for c in (0, 1):
                load(u, c).wait()

        @pl.when((i == tiles - 1) & (u + 1 < len(UNITS)))
        def _():
            fetch(u + 1)

        work(u, i, *where(u), x_v, ins, outs, out_sem, scratch)

    lax.fori_loop(0, tiles * len(UNITS), step, None)
    for half in (0, 1):
        for part in range(PARTS):
            for i in range(len(SENDS)):
                link(part, half, i).wait_send()
    for u in range(len(UNITS)):
        pair(u).wait_send()
    work(None, None, *where(0), x_v, ins, outs, out_sem, scratch)


def _call_fetched(tiles, work, load_weights, t, ins, out_shapes, out_sems, scratch, collective_id, flops):
    rows, columns = t.shape
    anywhere = pl.BlockSpec(memory_space=pl.ANY)
    dma = pltpu.SemaphoreType.DMA
    got = pl.pallas_call(
        functools.partial(_fetched, tiles, work, load_weights, 1 + len(ins), len(out_shapes)),
        out_shape=[*out_shapes, jax.ShapeDtypeStruct((16, rows, columns), t.dtype)],
        in_specs=[anywhere] * (1 + len(ins)),
        out_specs=[anywhere] * (len(out_shapes) + 1),
        scratch_shapes=[pltpu.VMEM((2, 2, rows // 2, columns), t.dtype), dma((2, 2)), dma((2, PARTS, 7)), dma((2, PARTS, 7)), dma((16,)), dma((16,)),
                        dma(out_sems), *scratch],
        compiler_params=pltpu.CompilerParams(collective_id=collective_id, has_side_effects=True, vmem_limit_bytes=VMEM),
        cost_estimate=pl.CostEstimate(flops=flops, bytes_accessed=4 * 16 * rows * columns, transcendentals=0),
    )(t, *ins)
    return got[:-1]


TILE = 768
COLS = 768


def gated(t, w_gate, w_up, collective_id):
    rows, depth = t.shape
    columns = w_gate.shape[1]
    tiles = columns // TILE

    def weights(i, ins, w_v, w_sem):
        return [pltpu.make_async_copy(ins[k].at[:, pl.ds(i * TILE, TILE)], w_v.at[i, :, pl.ds(k * TILE, TILE)], w_sem.at[i, k]) for k in (0, 1)]

    def load_weights(ins, scratch):
        w_v, w_sem, o_v = scratch
        for i in range(tiles):
            for copy in weights(i, ins, w_v, w_sem):
                copy.start()

    def work(u, i, source, half, x_v, ins, outs, out_sem, scratch):
        w_v, w_sem, o_v = scratch

        def out(u):
            slot = lax.rem(u, 2)
            return pltpu.make_async_copy(o_v.at[slot], outs[0].at[pl.ds(source * 2, 2), pl.ds(half * (rows // 2), rows // 2)], out_sem.at[slot])

        if u is None:
            out(0).wait()
            out(1).wait()
            return

        @pl.when(u == 0)
        def _():
            for copy in weights(i, ins, w_v, w_sem):
                copy.wait()

        @pl.when((i == 0) & (u >= 2))
        def _():
            out(u).wait()

        slot = lax.rem(u, 2)
        both = jnp.dot(x_v[slot].reshape(rows, depth), w_v[i], preferred_element_type=jnp.float32)
        gate, up = both[:, :TILE], both[:, TILE:]
        made = (gate * jax.nn.sigmoid(gate) * up).astype(jnp.bfloat16)
        o_v[slot, :, :, pl.ds(pl.multiple_of(i * TILE, TILE), TILE)] = made.reshape(2, rows // 2, TILE)

        @pl.when(i == tiles - 1)
        def _():
            out(u).start()

    scratch = [pltpu.VMEM((tiles, depth, 2 * TILE), t.dtype), pltpu.SemaphoreType.DMA((tiles, 2)), pltpu.VMEM((2, 2, rows // 2, columns), t.dtype)]
    return _call_fetched(tiles, work, load_weights, t, [w_gate, w_up], [jax.ShapeDtypeStruct((16, rows, columns), t.dtype)], (2,), scratch,
                         collective_id, 4 * 16 * rows * depth * columns)[0]


def _angles(rows, theta):
    half = HEAD // 2
    place = jnp.concatenate([128 * jnp.arange(rows // 128), jnp.arange(128)]).astype(jnp.float32)
    angle = place[:, None] * theta ** (-jnp.arange(half, dtype=jnp.float32) / half)
    cos, sin = jnp.cos(angle), jnp.sin(angle)
    return jnp.concatenate([cos, cos], 1), jnp.concatenate([-sin, sin], 1)


def projected(t, wq, wk, wv, collective_id):
    rows, depth = t.shape
    heads = [w.shape[1] // HEAD for w in (wq, wk, wv)]
    total = sum(heads)
    half_rows = rows // 2

    def loads(ins, scratch):
        w_v, cos_v, sin_v, w_sem = scratch[:4]
        at, copies = 0, []
        for k in range(3):
            copies.append(pltpu.make_async_copy(ins[k], w_v.at[:, pl.ds(at, ins[k].shape[1])], w_sem.at[k]))
            at += ins[k].shape[1]
        return copies + [pltpu.make_async_copy(ins[3], cos_v, w_sem.at[3]), pltpu.make_async_copy(ins[4], sin_v, w_sem.at[4])]

    def load_weights(ins, scratch):
        for copy in loads(ins, scratch):
            copy.start()

    def work(u, i, source, half, x_v, ins, outs, out_sem, scratch):
        w_v, cos_v, sin_v, w_sem, o_v = scratch

        def out(u):
            slot, at, copies = lax.rem(u, 2), 0, []
            for k in range(3):
                to = outs[k].at[:, pl.ds(source * 2, 2), pl.ds(half * half_rows, half_rows)]
                copies.append(pltpu.make_async_copy(o_v.at[slot, pl.ds(at, heads[k])], to, out_sem.at[slot, k]))
                at += heads[k]
            return copies

        if u is None:
            for copy in out(0) + out(1):
                copy.wait()
            return

        @pl.when(u == 0)
        def _():
            for copy in loads(ins, scratch):
                copy.wait()

        @pl.when(u >= 2)
        def _():
            for copy in out(u):
                copy.wait()

        slot = lax.rem(u, 2)
        made = jnp.dot(x_v[slot].reshape(rows, depth), w_v[...], preferred_element_type=jnp.float32).astype(jnp.bfloat16)
        near = pl.ds(cos_v.shape[0] - 128, 128)
        cos_b, sin_b = cos_v[near, :], sin_v[near, :]
        for c in (0, 1):
            far = pl.ds((source * 2 + c) * (rows // 128) + half, 1)
            cos_a, sin_a = cos_v[far, :], sin_v[far, :]
            cos, sin = cos_a * cos_b - sin_a * sin_b, sin_a * cos_b + cos_a * sin_b
            for n in range(total):
                head = made[c * half_rows : (c + 1) * half_rows, n * HEAD : (n + 1) * HEAD]
                if n < heads[0] + heads[1]:
                    wide = head.astype(jnp.float32)
                    head = (wide * cos + pltpu.roll(wide, HEAD // 2, 1) * sin).astype(jnp.bfloat16)
                o_v[slot, n, c] = head
        for copy in out(u):
            copy.start()

    cos, sin = _angles(16 * rows, THETA)
    scratch = [pltpu.VMEM((depth, total * HEAD), t.dtype), pltpu.VMEM(cos.shape, jnp.float32), pltpu.VMEM(cos.shape, jnp.float32),
               pltpu.SemaphoreType.DMA((5,)), pltpu.VMEM((2, total, 2, half_rows, HEAD), t.dtype)]
    return _call_fetched(1, work, load_weights, t, [wq, wk, wv, cos, sin], [jax.ShapeDtypeStruct((n, 16, rows, HEAD), t.dtype) for n in heads], (2, 3),
                         scratch, collective_id, 2 * 16 * rows * depth * total * HEAD)


def solution(mesh):
    def plus(t, y):
        return (t.astype(jnp.float32) + y.astype(jnp.float32)).astype(jnp.bfloat16)

    def step(x, gain_a, wq, wk, wv, wo, gain_m, w_gate, w_up, w_down):
        h = plus(x, summed(projected(normed(x, gain_a), wq, wk, wv, 2), wo, 0, 512))
        return plus(h, summed((gated(normed(h, gain_m), w_gate, w_up, 3),), w_down, 1, COLS))

    tokens, columns, rows_of = P(("dp", "tp"), None), P(None, "tp"), P("tp", None)
    return jax.shard_map(
        step,
        mesh=mesh,
        in_specs=(tokens, P(None), columns, columns, columns, rows_of, P(None), columns, columns, rows_of),
        out_specs=tokens,
        check_vma=False,
    )
```
